16 devices in a mesh: my: 4 (over z, y), mx: 4 (over x, core).
Axes of the slice: x: 2, y: 2, z: 2, core: 2. Of those that a mesh axis runs over, the one named last changes fastest.
Arguments:
- x_in: bfloat16 [512, 3584], P(None, 'mx')
- seq_lens: int32 [512], P('mx')
- gain_attn: bfloat16 [3584], P('mx')
- gain_mlp: bfloat16 [3584], P('mx')
- w_q: bfloat16 [3584, 3584], P('mx', 'my')
- b_q: bfloat16 [3584], P('my')
- w_k: bfloat16 [3584, 512], P('mx', 'my')
- b_k: bfloat16 [512], P('my')
- w_v: bfloat16 [3584, 512], P('mx', 'my')
- b_v: bfloat16 [512], P('my')
- w_o: bfloat16 [3584, 3584], P('my', 'mx')
- w_gate: bfloat16 [3584, 18944], P('mx', 'my')
- w_up: bfloat16 [3584, 18944], P('mx', 'my')
- w_down: bfloat16 [18944, 3584], P('my', 'mx')
- k_cache: bfloat16 [512, 512, 4, 128], P('mx', None, 'my')
- v_cache: bfloat16 [512, 512, 4, 128], P('mx', None, 'my')
Outputs:
- output 1: bfloat16 [512, 3584], P(None, 'mx')
- output 2: bfloat16 [512, 512, 4, 128], P('mx', None, 'my')
- output 3: bfloat16 [512, 512, 4, 128], P('mx', None, 'my')
All inputs are finite; a program needn't handle non-finite values.
Results may differ from the reference program's by a relative error of at most 0.0170983.
Values are sent between devices in bfloat16 or wider.
A program may use at most 1 GiB of HBM per device.

```python
import jax
import jax.numpy as jnp
from jax import lax

D = 3584
HEADS = 28
KV_HEADS = 4
HEAD = 128
FF = 18944
BATCH = 512
SEQ = 512
NORM_EPS = 1e-6
ROPE_THETA = 1000000.0
GROUP = HEADS // KV_HEADS


def setup_inputs(seed: int = 0) -> dict:
    key_list = jax.random.split(jax.random.key(seed), 17)
    q_width = HEADS * HEAD
    kv_width = KV_HEADS * HEAD
    cache_shape = (BATCH, SEQ, KV_HEADS, HEAD)

    def normal(key_index, shape, scale, offset=0.0):
        samples = jax.random.normal(key_list[key_index], shape, jnp.float32)
        return (offset + scale * samples).astype(jnp.bfloat16)

    lens_draw = jax.random.randint(key_list[0], (BATCH,), 0, SEQ)
    full_row = jax.random.randint(key_list[1], (), 0, BATCH)
    seq_lens = jnp.where(jnp.arange(BATCH) == full_row, SEQ - 1, lens_draw).astype(jnp.int32)
    return {
        "x_in": normal(2, (BATCH, D), 1.0),
        "seq_lens": seq_lens,
        "gain_attn": normal(3, (D,), 0.3, 1.0),
        "gain_mlp": normal(4, (D,), 0.3, 1.0),
        "w_q": normal(5, (D, q_width), 2.0 * D ** -0.5),
        "b_q": normal(6, (q_width,), 1.0),
        "w_k": normal(7, (D, kv_width), D ** -0.5),
        "b_k": normal(8, (kv_width,), 1.0),
        "w_v": normal(9, (D, kv_width), D ** -0.5),
        "b_v": normal(10, (kv_width,), 1.0),
        "w_o": normal(11, (q_width, D), q_width ** -0.5),
        "w_gate": normal(12, (D, FF), D ** -0.5),
        "w_up": normal(13, (D, FF), D ** -0.5),
        "w_down": normal(14, (FF, D), FF ** -0.5),
        "k_cache": normal(15, cache_shape, 1.0),
        "v_cache": normal(16, cache_shape, 1.0),
    }


def rms_norm(rows_in, gain_vec):
    rows_f32 = rows_in.astype(jnp.float32)
    mean_sq = jnp.mean(rows_f32 * rows_f32, axis=-1, keepdims=True)
    return (rows_f32 * lax.rsqrt(mean_sq + NORM_EPS) * gain_vec.astype(jnp.float32)).astype(jnp.bfloat16)


def apply_rotary(vectors, positions):
    half_dim = HEAD // 2
    inv_freq = ROPE_THETA ** (-2.0 * jnp.arange(half_dim, dtype=jnp.float32) / HEAD)
    angles = positions.astype(jnp.float32)[:, None, None] * inv_freq
    cos_tab = jnp.cos(angles)
    sin_tab = jnp.sin(angles)
    lower_half = vectors[..., :half_dim]
    upper_half = vectors[..., half_dim:]
    return jnp.concatenate([lower_half * cos_tab - upper_half * sin_tab, upper_half * cos_tab + lower_half * sin_tab], axis=-1)


def attend_one(row_inputs):
    q_row, k_rows, v_rows, length = row_inputs
    q_grouped = q_row.reshape(KV_HEADS, GROUP, HEAD).astype(jnp.float32)
    scores = jnp.einsum("kgd,skd->kgs", q_grouped, k_rows.astype(jnp.float32)) * HEAD ** -0.5
    visible = (jnp.arange(SEQ) <= length)[None, None, :]
    scores = jnp.where(visible, scores, -jnp.inf)
    weights = jnp.exp(scores - jnp.max(scores, axis=-1, keepdims=True))
    weight_sum = jnp.sum(weights, axis=-1, keepdims=True)
    weighted = jnp.einsum("kgs,skd->kgd", weights.astype(jnp.bfloat16).astype(jnp.float32), v_rows.astype(jnp.float32))
    return (weighted / weight_sum).astype(jnp.bfloat16).reshape(HEADS * HEAD)


def reference(x_in, seq_lens, gain_attn, gain_mlp, w_q, b_q, w_k, b_k, w_v, b_v, w_o, w_gate, w_up, w_down, k_cache, v_cache):
    normed = rms_norm(x_in, gain_attn)
    q_vals = jnp.dot(normed, w_q, preferred_element_type=jnp.float32) + b_q.astype(jnp.float32)
    k_vals = jnp.dot(normed, w_k, preferred_element_type=jnp.float32) + b_k.astype(jnp.float32)
    v_vals = jnp.dot(normed, w_v, preferred_element_type=jnp.float32) + b_v.astype(jnp.float32)
    q_rot = apply_rotary(q_vals.reshape(BATCH, HEADS, HEAD), seq_lens).astype(jnp.bfloat16)
    k_rot = apply_rotary(k_vals.reshape(BATCH, KV_HEADS, HEAD), seq_lens).astype(jnp.bfloat16)
    v_new = v_vals.reshape(BATCH, KV_HEADS, HEAD).astype(jnp.bfloat16)
    at_slot = (jnp.arange(SEQ)[None, :] == seq_lens[:, None])[:, :, None, None]
    k_cache_out = jnp.where(at_slot, k_rot[:, None], k_cache)
    v_cache_out = jnp.where(at_slot, v_new[:, None], v_cache)
    attn_rows = lax.map(attend_one, (q_rot, k_cache_out, v_cache_out, seq_lens))
    x_mid = (x_in.astype(jnp.float32) + jnp.dot(attn_rows, w_o, preferred_element_type=jnp.float32)).astype(jnp.bfloat16)
    normed_mlp = rms_norm(x_mid, gain_mlp)
    gate_proj = jnp.dot(normed_mlp, w_gate, preferred_element_type=jnp.float32)
    up_proj = jnp.dot(normed_mlp, w_up, preferred_element_type=jnp.float32)
    hidden_act = (jax.nn.silu(gate_proj) * up_proj).astype(jnp.bfloat16)
    x_out = (x_mid.astype(jnp.float32) + jnp.dot(hidden_act, w_down, preferred_element_type=jnp.float32)).astype(jnp.bfloat16)
    return (x_out, k_cache_out, v_cache_out)
```

```python
import jax
import jax.numpy as jnp
from jax import lax
from jax.experimental import pallas as pl
from jax.experimental.pallas import tpu as pltpu
from jax.sharding import PartitionSpec as P

HEAD = 128
NORM_EPS = 1e-6
ROPE_THETA = 1000000.0
CHUNKS = 4
MESH_IDS = pl.DeviceIdType.MESH


def over_tiles(total, tile, body):
    count = total // tile

    def step(i, carry):
        body(pl.multiple_of(i * tile, tile), tile)
        return carry

    lax.fori_loop(0, count, step, 0)
    if total % tile:
        body(count * tile, total % tile)


def mx_peers():
    me = lax.axis_index("mx")
    core = lax.rem(me, 2)
    sib = me + 1 - 2 * core
    return me, sib, lax.rem(me + 2, 4), lax.rem(sib + 2, 4)


def my_peers():
    me = lax.axis_index("my")
    flip = me + 1 - 2 * lax.rem(me, 2)
    return me, (flip, lax.rem(me + 2, 4), lax.rem(flip + 2, 4))


def column_to_lanes(col):
    rows = col.shape[0]
    return jnp.transpose(jnp.broadcast_to(col, (rows, rows)))[:8]


def lanes_to_column(lanes):
    width = lanes.shape[1]
    return jnp.transpose(jnp.broadcast_to(lanes[:1], (width, width)))


def enter(axis_peers):
    barrier = pltpu.get_barrier_semaphore()
    for axis, peer in axis_peers:
        pl.semaphore_signal(barrier, inc=1, device_id={axis: peer}, device_id_type=MESH_IDS)
    pl.semaphore_wait(barrier, len(axis_peers))


def mlp_kernel(attn, x_in, gain, w_o, w_gate, w_up, w_down, out,
               wo_v, wg_v, wu_v, wd_v, x_v, attn_all, o_part, o_recv, mid, stat_send, stat_recv, h2,
               part, pair_recv, cross_send, cross_recv, act, acc, d_part, d_recv, out_all,
               w_sem, s_gather, r_gather, s_red, r_red, s_bc, r_bc, s_stat, r_stat, s_pair, r_pair,
               s_cross, r_cross, s_act, r_act, s_red2, r_red2, s_bc2, r_bc2, out_sem):
    mx, sib, across, across_sib = mx_peers()
    my, my_list = my_peers()
    rb = mid.shape[2]
    hid = mid.shape[3]
    ff = wg_v.shape[1]
    rows = 4 * rb

    def remote(src, dst, send, recv, axis, peer):
        return pltpu.make_async_remote_copy(src_ref=src, dst_ref=dst, send_sem=send, recv_sem=recv, device_id={axis: peer}, device_id_type=MESH_IDS)

    loads = [
        pltpu.make_async_copy(w_o, wo_v, w_sem.at[0]),
        pltpu.make_async_copy(x_in.at[pl.ds(pl.multiple_of(my * CHUNKS * rb, CHUNKS * rb), CHUNKS * rb)], x_v, w_sem.at[1]),
        pltpu.make_async_copy(w_gate, wg_v, w_sem.at[2]),
        pltpu.make_async_copy(w_up, wu_v, w_sem.at[3]),
        pltpu.make_async_copy(w_down, wd_v, w_sem.at[4]),
    ]
    for load in loads:
        load.start()
    enter([("mx", sib), ("mx", across), ("mx", across_sib)] + [("my", p) for p in my_list])

    def gather_copies(k):
        src = attn.at[pl.ds(k * rb, rb)]
        return (remote(src, attn_all.at[k, mx], s_gather.at[k, 0], r_gather.at[k, 0], "mx", across),
                remote(src, attn_all.at[k, mx], s_gather.at[k, 1], r_gather.at[k, 1], "mx", sib),
                remote(attn_all.at[k, across], attn_all.at[k, across], s_gather.at[k, 2], r_gather.at[k, 2], "mx", sib))

    def reduce_copies(k, src, dst, send, recv):
        return [remote(src.at[k, p], dst.at[k, d], send.at[k, d], recv.at[k, d], "my", p) for d, p in enumerate(my_list)]

    def bcast_copies(k, buf, send, recv):
        return [remote(buf.at[k, my], buf.at[k, my], send.at[k, d], recv.at[k, d], "my", p) for d, p in enumerate(my_list)]

    def stat_copies(k):
        return [remote(stat_send.at[k], stat_recv.at[k, d], s_stat.at[k, d], r_stat.at[k, d], "mx", p) for d, p in enumerate((sib, across, across_sib))]

    def pair_copies(k):
        return [remote(part.at[k, across_sib], pair_recv.at[k, 0], s_pair.at[k, 0], r_pair.at[k, 0], "mx", sib),
                remote(part.at[k, sib], pair_recv.at[k, 1], s_pair.at[k, 1], r_pair.at[k, 1], "mx", sib)]

    def cross_copy(k):
        return remote(cross_send.at[k], cross_recv.at[k], s_cross.at[k], r_cross.at[k], "mx", across)

    def act_copies(k):
        return (remote(act.at[k, mx], act.at[k, mx], s_act.at[k, 0], r_act.at[k, 0], "mx", across),
                remote(act.at[k, mx], act.at[k, mx], s_act.at[k, 1], r_act.at[k, 1], "mx", sib),
                remote(act.at[k, across], act.at[k, across], s_act.at[k, 2], r_act.at[k, 2], "mx", sib))

    def start_gather(k):
        to_across, to_sib, _ = gather_copies(k)
        to_across.start()
        to_sib.start()
        attn_all[k, mx] = attn[pl.ds(k * rb, rb), :]

    def forward_gather(k):
        to_across, _, forward = gather_copies(k)
        to_across.wait_recv()
        forward.start()

    def out_proj(k):
        _, to_sib, forward = gather_copies(k)
        to_sib.wait_recv()
        forward.wait_recv()
        if k == 0:
            loads[0].wait()
        rows_in = attn_all[k].reshape(rows, hid)
        o_part[k] = jnp.dot(rows_in, wo_v[...], preferred_element_type=jnp.float32).astype(jnp.bfloat16).reshape(4, rb, hid)
        for copy in reduce_copies(k, o_part, o_recv, s_red, r_red):
            copy.start()

    def own_block(k):
        for copy in reduce_copies(k, o_part, o_recv, s_red, r_red):
            copy.wait_recv()
        if k == 0:
            loads[1].wait()
        total = o_part[k, my].astype(jnp.float32)
        for d in range(3):
            total += o_recv[k, d].astype(jnp.float32)
        mid[k, my] = (x_v[k * rb:(k + 1) * rb].astype(jnp.float32) + total).astype(jnp.bfloat16)
        for copy in bcast_copies(k, mid, s_bc, r_bc):
            copy.start()

    def stats(k):
        for copy in bcast_copies(k, mid, s_bc, r_bc):
            copy.wait_recv()
        rows_f32 = mid[k].reshape(rows, hid).astype(jnp.float32)
        stat_send[k] = column_to_lanes(jnp.sum(rows_f32 * rows_f32, axis=1, keepdims=True))
        for copy in stat_copies(k):
            copy.start()

    def gate_up(k):
        for copy in stat_copies(k):
            copy.wait_recv()
        if k == 0:
            loads[2].wait()
            loads[3].wait()
        total = stat_send[k] + stat_recv[k, 0] + stat_recv[k, 1] + stat_recv[k, 2]
        scale = lanes_to_column(lax.rsqrt(total / (4 * hid) + NORM_EPS))
        gain_row = gain[...].astype(jnp.float32)
        for t in range(hid // 128):
            cols = slice(t * 128, (t + 1) * 128)
            piece = mid[k, :, :, cols].reshape(rows, 128).astype(jnp.float32)
            h2[:, cols] = (piece * scale * gain_row[:, cols]).astype(jnp.bfloat16)

        def body(off, tile):
            lhs = h2[...]
            part[k, :, :, pl.ds(off, tile)] = jnp.dot(lhs, wg_v[:, pl.ds(off, tile)], preferred_element_type=jnp.float32).astype(jnp.bfloat16).reshape(4, rb, tile)
            part[k, :, :, pl.ds(pl.multiple_of(off + ff, 128), tile)] = jnp.dot(lhs, wu_v[:, pl.ds(off, tile)], preferred_element_type=jnp.float32).astype(jnp.bfloat16).reshape(4, rb, tile)

        over_tiles(ff, 512, body)
        for copy in pair_copies(k):
            copy.start()

    def pair_sum(k):
        pair_copies(k)[0].wait_recv()

        def body(off, tile):
            cols = pl.ds(off, tile)
            cross_send[k, :, cols] = (part[k, across, :, cols].astype(jnp.float32) + pair_recv[k, 0, :, cols].astype(jnp.float32)).astype(jnp.bfloat16)

        over_tiles(2 * ff, 512, body)
        cross_copy(k).start()

    def activate(k):
        pair_copies(k)[1].wait_recv()
        cross_copy(k).wait_recv()

        def total(cols):
            return part[k, mx, :, cols].astype(jnp.float32) + pair_recv[k, 1, :, cols].astype(jnp.float32) + cross_recv[k, :, cols].astype(jnp.float32)

        def body(off, tile):
            gate = total(pl.ds(off, tile))
            up = total(pl.ds(pl.multiple_of(off + ff, 128), tile))
            act[k, mx, :, pl.ds(off, tile)] = (jax.nn.silu(gate) * up).astype(jnp.bfloat16)

        over_tiles(ff, 512, body)
        to_across, to_sib, _ = act_copies(k)
        to_across.start()
        to_sib.start()

    def forward_act(k):
        to_across, _, forward = act_copies(k)
        to_across.wait_recv()
        forward.start()

    def down(k):
        _, to_sib, forward = act_copies(k)
        to_sib.wait_recv()
        forward.wait_recv()
        if k == 0:
            loads[4].wait()
        acc[...] = jnp.zeros_like(acc)

        def body(off, tile):
            lhs = act[k, :, :, pl.ds(off, tile)].reshape(rows, tile)
            acc[...] += jnp.dot(lhs, wd_v[pl.ds(off, tile), :], preferred_element_type=jnp.float32)

        over_tiles(ff, 512, body)
        d_part[k] = acc[...].astype(jnp.bfloat16).reshape(4, rb, hid)
        for copy in reduce_copies(k, d_part, d_recv, s_red2, r_red2):
            copy.start()

    def out_block(k):
        for copy in reduce_copies(k, d_part, d_recv, s_red2, r_red2):
            copy.wait_recv()
        total = d_part[k, my].astype(jnp.float32)
        for d in range(3):
            total += d_recv[k, d].astype(jnp.float32)
        out_all[k, my] = (mid[k, my].astype(jnp.float32) + total).astype(jnp.bfloat16)
        for copy in bcast_copies(k, out_all, s_bc2, r_bc2):
            copy.start()

    def out_copies(k):
        return [pltpu.make_async_copy(out_all.at[k, j], out.at[pl.ds((j * CHUNKS + k) * rb, rb)], out_sem.at[k, j]) for j in range(4)]

    def write_out(k):
        for copy in bcast_copies(k, out_all, s_bc2, r_bc2):
            copy.wait_recv()
        for copy in out_copies(k):
            copy.start()

    for k in range(CHUNKS):
        start_gather(k)
    plan = [(forward_gather, 0), (out_proj, 0), (forward_gather, 1), (out_proj, 1), (own_block, 0), (own_block, 1), (stats, 0),
            (forward_gather, 2), (out_proj, 2), (gate_up, 0), (stats, 1), (pair_sum, 0), (gate_up, 1), (own_block, 2), (forward_gather, 3), (out_proj, 3),
            (pair_sum, 1), (stats, 2), (own_block, 3), (gate_up, 2), (stats, 3), (activate, 0), (pair_sum, 2), (gate_up, 3), (activate, 1), (pair_sum, 3),
            (forward_act, 0), (down, 0), (activate, 2), (forward_act, 1), (down, 1), (out_block, 0), (activate, 3), (out_block, 1), (write_out, 0),
            (forward_act, 2), (down, 2), (write_out, 1), (forward_act, 3), (down, 3), (out_block, 2), (out_block, 3), (write_out, 2), (write_out, 3)]
    for stage, k in plan:
        stage(k)

    for k in range(CHUNKS):
        sends = list(gather_copies(k)) + reduce_copies(k, o_part, o_recv, s_red, r_red) + bcast_copies(k, mid, s_bc, r_bc) + stat_copies(k)
        sends += pair_copies(k) + [cross_copy(k)] + list(act_copies(k))
        sends += reduce_copies(k, d_part, d_recv, s_red2, r_red2) + bcast_copies(k, out_all, s_bc2, r_bc2)
        for copy in sends:
            copy.wait_send()
        for copy in out_copies(k):
            copy.wait()


def mlp_call(attn, x_in, gain, w_o, w_gate, w_up, w_down):
    row_total, hid = x_in.shape
    ff = w_gate.shape[1]
    rb = row_total // (4 * CHUNKS)
    bf16 = jnp.bfloat16
    f32 = jnp.float32
    vmem = pl.BlockSpec(memory_space=pltpu.VMEM)
    hbm = pl.BlockSpec(memory_space=pl.ANY)
    dma = pltpu.SemaphoreType.DMA
    return pl.pallas_call(
        mlp_kernel,
        out_shape=jax.ShapeDtypeStruct((row_total, hid), bf16),
        in_specs=[vmem, hbm, vmem, hbm, hbm, hbm, hbm],
        out_specs=hbm,
        scratch_shapes=[
            pltpu.VMEM(w_o.shape, bf16), pltpu.VMEM(w_gate.shape, bf16), pltpu.VMEM(w_up.shape, bf16), pltpu.VMEM(w_down.shape, bf16),
            pltpu.VMEM((CHUNKS * rb, hid), bf16),
            pltpu.VMEM((CHUNKS, 4, rb, hid), bf16),
            pltpu.VMEM((CHUNKS, 4, rb, hid), bf16), pltpu.VMEM((CHUNKS, 3, rb, hid), bf16),
            pltpu.VMEM((CHUNKS, 4, rb, hid), bf16),
            pltpu.VMEM((CHUNKS, 8, 4 * rb), f32), pltpu.VMEM((CHUNKS, 3, 8, 4 * rb), f32),
            pltpu.VMEM((4 * rb, hid), bf16),
            pltpu.VMEM((CHUNKS, 4, rb, 2 * ff), bf16), pltpu.VMEM((CHUNKS, 2, rb, 2 * ff), bf16),
            pltpu.VMEM((CHUNKS, rb, 2 * ff), bf16), pltpu.VMEM((CHUNKS, rb, 2 * ff), bf16),
            pltpu.VMEM((CHUNKS, 4, rb, ff), bf16),
            pltpu.VMEM((4 * rb, hid), f32),
            pltpu.VMEM((CHUNKS, 4, rb, hid), bf16), pltpu.VMEM((CHUNKS, 3, rb, hid), bf16),
            pltpu.VMEM((CHUNKS, 4, rb, hid), bf16),
            dma((5,)),
            dma((CHUNKS, 3)), dma((CHUNKS, 3)), dma((CHUNKS, 3)), dma((CHUNKS, 3)), dma((CHUNKS, 3)), dma((CHUNKS, 3)),
            dma((CHUNKS, 3)), dma((CHUNKS, 3)), dma((CHUNKS, 2)), dma((CHUNKS, 2)),
            dma((CHUNKS,)), dma((CHUNKS,)), dma((CHUNKS, 3)), dma((CHUNKS, 3)),
            dma((CHUNKS, 3)), dma((CHUNKS, 3)), dma((CHUNKS, 3)), dma((CHUNKS, 3)), dma((CHUNKS, 4)),
        ],
        compiler_params=pltpu.CompilerParams(collective_id=1, has_side_effects=True, vmem_limit_bytes=67043328),
        name="attn_out_mlp",
    )(attn, x_in, gain.reshape(1, hid), w_o, w_gate, w_up, w_down)


def apply_rotary(vectors, positions):
    half_dim = HEAD // 2
    inv_freq = ROPE_THETA ** (-2.0 * jnp.arange(half_dim, dtype=jnp.float32) / HEAD)
    angles = positions.astype(jnp.float32)[:, None, None] * inv_freq
    cos_tab = jnp.cos(angles)
    sin_tab = jnp.sin(angles)
    lower_half = vectors[..., :half_dim]
    upper_half = vectors[..., half_dim:]
    return jnp.concatenate([lower_half * cos_tab - upper_half * sin_tab, upper_half * cos_tab + lower_half * sin_tab], axis=-1)


def attend_local(q_rot, k_cache_out, v_cache_out, seq_lens):
    row_count, seq_len, kv_heads, _ = k_cache_out.shape
    q_heads = q_rot.shape[1]
    q_grouped = q_rot.reshape(row_count, kv_heads, q_heads // kv_heads, HEAD)
    scores = jnp.einsum("bkgd,bskd->bkgs", q_grouped, k_cache_out, preferred_element_type=jnp.float32) * HEAD ** -0.5
    visible = (jnp.arange(seq_len)[None, :] <= seq_lens[:, None])[:, None, None, :]
    scores = jnp.where(visible, scores, -jnp.inf)
    weights = jnp.exp(scores - jnp.max(scores, axis=-1, keepdims=True))
    weight_sum = jnp.sum(weights, axis=-1, keepdims=True)
    weighted = jnp.einsum("bkgs,bskd->bkgd", weights.astype(jnp.bfloat16), v_cache_out, preferred_element_type=jnp.float32)
    return (weighted / weight_sum).astype(jnp.bfloat16).reshape(row_count, q_heads * HEAD)


def solution(mesh):
    mx_size = mesh.shape["mx"]
    act_spec = P(None, "mx")
    cache_spec = P("mx", None, "my", None)
    in_specs = (act_spec, P("mx"), P("mx"), P("mx"), P("mx", "my"), P("my"), P("mx", "my"), P("my"), P("mx", "my"), P("my"), P("my", "mx"), P("mx", "my"), P("mx", "my"), P("my", "mx"), cache_spec, cache_spec)
    out_specs = (act_spec, cache_spec, cache_spec)

    def local_layer(x_in, seq_lens, gain_attn, gain_mlp, w_q, b_q, w_k, b_k, w_v, b_v, w_o, w_gate, w_up, w_down, k_cache, v_cache):
        hidden = x_in.shape[1] * mx_size
        x_f32 = x_in.astype(jnp.float32)
        attn_sq = lax.psum(jnp.sum(x_f32 * x_f32, axis=1, keepdims=True), "mx")
        normed = (x_f32 * lax.rsqrt(attn_sq / hidden + NORM_EPS) * gain_attn.astype(jnp.float32)).astype(jnp.bfloat16)
        q_cols = w_q.shape[1]
        kv_cols = w_k.shape[1]
        partials = jnp.concatenate([
            jnp.dot(normed, w_q, preferred_element_type=jnp.float32).astype(jnp.bfloat16),
            jnp.dot(normed, w_k, preferred_element_type=jnp.float32).astype(jnp.bfloat16),
            jnp.dot(normed, w_v, preferred_element_type=jnp.float32).astype(jnp.bfloat16),
        ], axis=1)
        projected = lax.psum_scatter(partials, "mx", scatter_dimension=0, tiled=True).astype(jnp.float32)
        row_count = projected.shape[0]
        kv_heads = kv_cols // HEAD
        q_vals = projected[:, :q_cols] + b_q.astype(jnp.float32)
        k_vals = projected[:, q_cols:q_cols + kv_cols] + b_k.astype(jnp.float32)
        v_vals = projected[:, q_cols + kv_cols:] + b_v.astype(jnp.float32)
        q_rot = apply_rotary(q_vals.reshape(row_count, q_cols // HEAD, HEAD), seq_lens).astype(jnp.bfloat16)
        k_rot = apply_rotary(k_vals.reshape(row_count, kv_heads, HEAD), seq_lens).astype(jnp.bfloat16)
        v_new = v_vals.reshape(row_count, kv_heads, HEAD).astype(jnp.bfloat16)
        at_slot = (jnp.arange(k_cache.shape[1])[None, :] == seq_lens[:, None])[:, :, None, None]
        k_cache_out = jnp.where(at_slot, k_rot[:, None], k_cache)
        v_cache_out = jnp.where(at_slot, v_new[:, None], v_cache)
        attn_rows = attend_local(q_rot, k_cache_out, v_cache_out, seq_lens)
        x_out = mlp_call(attn_rows, x_in, gain_mlp, w_o, w_gate, w_up, w_down)
        return x_out, k_cache_out, v_cache_out

    return jax.shard_map(local_layer, mesh=mesh, in_specs=in_specs, out_specs=out_specs, check_vma=False)
```

```python
import math

import jax
import jax.numpy as jnp
from jax import lax
from jax.experimental import pallas as pl
from jax.experimental.pallas import tpu as pltpu
from jax.sharding import PartitionSpec as P

HEAD = 128
NORM_EPS = 1e-6
ROPE_THETA = 1000000.0
VMEM_BYTES = 67043328
CHUNKS = 4
PLAN = ((0, 0), (1, 0), (0, 1), (1, 1), (2, 0), (2, 1), (3, 0), (0, 2), (1, 2), (4, 0), (3, 1), (5, 0), (4, 1), (2, 2), (0, 3), (1, 3), (5, 1), (3, 2), (2, 3), (4, 2), (3, 3), (6, 0), (5, 2), (4, 3), (6, 1), (5, 3), (7, 0), (8, 0), (6, 2), (7, 1), (8, 1), (9, 0), (6, 3), (9, 1), (10, 0), (7, 2), (8, 2), (10, 1), (7, 3), (8, 3), (9, 2), (9, 3), (10, 2), (10, 3))
MESH_IDS = pl.DeviceIdType.MESH


def over_tiles(total, tile, body):
    count = total // tile

    def step(i, carry):
        body(pl.multiple_of(i * tile, tile), tile)
        return carry

    lax.fori_loop(0, count, step, 0)
    if total % tile:
        body(count * tile, total % tile)


def mx_peers():
    me = lax.axis_index("mx")
    core = lax.rem(me, 2)
    sib = me + 1 - 2 * core
    return me, sib, lax.rem(me + 2, 4), lax.rem(sib + 2, 4)


def my_peers():
    me = lax.axis_index("my")
    flip = me + 1 - 2 * lax.rem(me, 2)
    return me, (flip, lax.rem(me + 2, 4), lax.rem(flip + 2, 4))


def column_to_lanes(col):
    wide = jnp.broadcast_to(col, (col.shape[0], 128))
    if col.shape[0] < 128:
        wide = jnp.concatenate([wide] * (128 // col.shape[0]), axis=0)
    return jnp.transpose(wide)[:8]


def lanes_to_column(lanes):
    return jnp.transpose(jnp.broadcast_to(lanes[:1], (128, 128)))


def enter(axis_peers):
    barrier = pltpu.get_barrier_semaphore()
    for axis, peer in axis_peers:
        pl.semaphore_signal(barrier, inc=1, device_id={axis: peer}, device_id_type=MESH_IDS)
    pl.semaphore_wait(barrier, len(axis_peers))


def mlp_kernel(attn_hbm, x_in, gain_hbm, w_o, w_gate, w_up, w_down, out,
               attn, gain, wo_v, wg_v, wu_v, wd_v, x_v, attn_all, o_part, o_recv, mid, stat_send, stat_recv, h2,
               part, pair_recv, cross_send, cross_recv, act, acc, d_part, d_recv, out_all,
               w_sem, s_gather, r_gather, s_red, r_red, s_bc, r_bc, s_stat, r_stat, s_pair, r_pair,
               s_cross, r_cross, s_act, r_act, s_red2, r_red2, s_bc2, r_bc2, out_sem):
    mx, sib, across, across_sib = mx_peers()
    my, my_list = my_peers()
    rb = mid.shape[2]
    hid = mid.shape[3]
    ff = wg_v.shape[1]
    rows = 4 * rb

    def remote(src, dst, send, recv, axis, peer):
        return pltpu.make_async_remote_copy(src_ref=src, dst_ref=dst, send_sem=send, recv_sem=recv, device_id={axis: peer}, device_id_type=MESH_IDS)

    first_loads = [pltpu.make_async_copy(attn_hbm, attn, w_sem.at[5]), pltpu.make_async_copy(gain_hbm, gain, w_sem.at[6])]
    loads = [
        pltpu.make_async_copy(w_o, wo_v, w_sem.at[0]),
        pltpu.make_async_copy(x_in.at[pl.ds(pl.multiple_of(my * CHUNKS * rb, CHUNKS * rb), CHUNKS * rb)], x_v, w_sem.at[1]),
        pltpu.make_async_copy(w_gate, wg_v, w_sem.at[2]),
        pltpu.make_async_copy(w_up, wu_v, w_sem.at[3]),
        pltpu.make_async_copy(w_down, wd_v, w_sem.at[4]),
    ]
    for load in first_loads + loads:
        load.start()
    enter([("mx", sib), ("mx", across), ("mx", across_sib)] + [("my", p) for p in my_list])

    def gather_copies(k):
        src = attn.at[pl.ds(k * rb, rb)]
        return (remote(src, attn_all.at[k, mx], s_gather.at[k, 0], r_gather.at[k, 0], "mx", across),
                remote(src, attn_all.at[k, mx], s_gather.at[k, 1], r_gather.at[k, 1], "mx", sib),
                remote(attn_all.at[k, across], attn_all.at[k, across], s_gather.at[k, 2], r_gather.at[k, 2], "mx", sib))

    def reduce_copies(k, src, dst, send, recv):
        return [remote(src.at[k, p], dst.at[k, d], send.at[k, d], recv.at[k, d], "my", p) for d, p in enumerate(my_list)]

    def bcast_copies(k, buf, send, recv):
        return [remote(buf.at[k, my], buf.at[k, my], send.at[k, d], recv.at[k, d], "my", p) for d, p in enumerate(my_list)]

    def stat_copies(k):
        return [remote(stat_send.at[k], stat_recv.at[k, d], s_stat.at[k, d], r_stat.at[k, d], "mx", p) for d, p in enumerate((sib, across, across_sib))]

    def pair_copies(k):
        return [remote(part.at[k, across_sib], pair_recv.at[k, 0], s_pair.at[k, 0], r_pair.at[k, 0], "mx", sib),
                remote(part.at[k, sib], pair_recv.at[k, 1], s_pair.at[k, 1], r_pair.at[k, 1], "mx", sib)]

    def cross_copy(k):
        return remote(cross_send.at[k], cross_recv.at[k], s_cross.at[k], r_cross.at[k], "mx", across)

    def act_copies(k):
        return (remote(act.at[k, mx], act.at[k, mx], s_act.at[k, 0], r_act.at[k, 0], "mx", across),
                remote(act.at[k, mx], act.at[k, mx], s_act.at[k, 1], r_act.at[k, 1], "mx", sib),
                remote(act.at[k, across], act.at[k, across], s_act.at[k, 2], r_act.at[k, 2], "mx", sib))

    def start_gather(k):
        to_across, to_sib, _ = gather_copies(k)
        to_across.start()
        to_sib.start()
        attn_all[k, mx] = attn[pl.ds(k * rb, rb), :]

    def forward_gather(k):
        to_across, _, forward = gather_copies(k)
        to_across.wait_recv()
        forward.start()

    def out_proj(k):
        _, to_sib, forward = gather_copies(k)
        to_sib.wait_recv()
        forward.wait_recv()
        if k == 0:
            loads[0].wait()
        rows_in = attn_all[k].reshape(rows, hid)
        o_part[k] = jnp.dot(rows_in, wo_v[...], preferred_element_type=jnp.float32).astype(jnp.bfloat16).reshape(4, rb, hid)
        for copy in reduce_copies(k, o_part, o_recv, s_red, r_red):
            copy.start()

    def own_block(k):
        for copy in reduce_copies(k, o_part, o_recv, s_red, r_red):
            copy.wait_recv()
        if k == 0:
            loads[1].wait()
        total = o_part[k, my].astype(jnp.float32)
        for d in range(3):
            total += o_recv[k, d].astype(jnp.float32)
        mid[k, my] = (x_v[k * rb:(k + 1) * rb].astype(jnp.float32) + total).astype(jnp.bfloat16)
        for copy in bcast_copies(k, mid, s_bc, r_bc):
            copy.start()

    def stats(k):
        for copy in bcast_copies(k, mid, s_bc, r_bc):
            copy.wait_recv()
        rows_f32 = mid[k].reshape(rows, hid).astype(jnp.float32)
        stat_send[k] = column_to_lanes(jnp.sum(rows_f32 * rows_f32, axis=1, keepdims=True))
        for copy in stat_copies(k):
            copy.start()

    def gate_up(k):
        for copy in stat_copies(k):
            copy.wait_recv()
        if k == 0:
            loads[2].wait()
            loads[3].wait()
        total = stat_send[k] + stat_recv[k, 0] + stat_recv[k, 1] + stat_recv[k, 2]
        scale = lanes_to_column(lax.rsqrt(total / (4 * hid) + NORM_EPS))[:rows]
        gain_rows = gain[...].astype(jnp.float32)
        for t in range(hid // 128):
            cols = slice(t * 128, (t + 1) * 128)
            piece = mid[k, :, :, cols].reshape(rows, 128).astype(jnp.float32)
            h2[:, cols] = (piece * scale * gain_rows[t:t + 1]).astype(jnp.bfloat16)

        def body(off, tile):
            lhs = h2[...]
            part[k, :, :, pl.ds(off, tile)] = jnp.dot(lhs, wg_v[:, pl.ds(off, tile)], preferred_element_type=jnp.float32).astype(jnp.bfloat16).reshape(4, rb, tile)
            part[k, :, :, pl.ds(pl.multiple_of(off + ff, 128), tile)] = jnp.dot(lhs, wu_v[:, pl.ds(off, tile)], preferred_element_type=jnp.float32).astype(jnp.bfloat16).reshape(4, rb, tile)

        over_tiles(ff, 512, body)
        for copy in pair_copies(k):
            copy.start()

    def pair_sum(k):
        pair_copies(k)[0].wait_recv()

        def body(off, tile):
            cols = pl.ds(off, tile)
            cross_send[k, :, cols] = (part[k, across, :, cols].astype(jnp.float32) + pair_recv[k, 0, :, cols].astype(jnp.float32)).astype(jnp.bfloat16)

        over_tiles(2 * ff, 512, body)
        cross_copy(k).start()

    def activate(k):
        pair_copies(k)[1].wait_recv()
        cross_copy(k).wait_recv()

        def total(cols):
            return part[k, mx, :, cols].astype(jnp.float32) + pair_recv[k, 1, :, cols].astype(jnp.float32) + cross_recv[k, :, cols].astype(jnp.float32)

        def body(off, tile):
            gate = total(pl.ds(off, tile))
            up = total(pl.ds(pl.multiple_of(off + ff, 128), tile))
            act[k, mx, :, pl.ds(off, tile)] = (jax.nn.silu(gate) * up).astype(jnp.bfloat16)

        over_tiles(ff, 512, body)
        to_across, to_sib, _ = act_copies(k)
        to_across.start()
        to_sib.start()

    def forward_act(k):
        to_across, _, forward = act_copies(k)
        to_across.wait_recv()
        forward.start()

    def down(k):
        _, to_sib, forward = act_copies(k)
        to_sib.wait_recv()
        forward.wait_recv()
        if k == 0:
            loads[4].wait()
        acc[...] = jnp.zeros_like(acc)

        def body(off, tile):
            lhs = act[k, :, :, pl.ds(off, tile)].reshape(rows, tile)
            acc[...] += jnp.dot(lhs, wd_v[pl.ds(off, tile), :], preferred_element_type=jnp.float32)

        over_tiles(ff, 512, body)
        d_part[k] = acc[...].astype(jnp.bfloat16).reshape(4, rb, hid)
        for copy in reduce_copies(k, d_part, d_recv, s_red2, r_red2):
            copy.start()

    def out_block(k):
        for copy in reduce_copies(k, d_part, d_recv, s_red2, r_red2):
            copy.wait_recv()
        total = d_part[k, my].astype(jnp.float32)
        for d in range(3):
            total += d_recv[k, d].astype(jnp.float32)
        out_all[k, my] = (mid[k, my].astype(jnp.float32) + total).astype(jnp.bfloat16)
        for copy in bcast_copies(k, out_all, s_bc2, r_bc2):
            copy.start()

    def out_copies(k):
        return [pltpu.make_async_copy(out_all.at[k, j], out.at[pl.ds((j * CHUNKS + k) * rb, rb)], out_sem.at[k, j]) for j in range(4)]

    def write_out(k):
        for copy in bcast_copies(k, out_all, s_bc2, r_bc2):
            copy.wait_recv()
        for copy in out_copies(k):
            copy.start()

    for load in first_loads:
        load.wait()
    for k in range(CHUNKS):
        start_gather(k)
    stages = (forward_gather, out_proj, own_block, stats, gate_up, pair_sum, activate, forward_act, down, out_block, write_out)
    for stage, k in PLAN:
        stages[stage](k)

    for k in range(CHUNKS):
        sends = list(gather_copies(k)) + reduce_copies(k, o_part, o_recv, s_red, r_red) + bcast_copies(k, mid, s_bc, r_bc) + stat_copies(k)
        sends += pair_copies(k) + [cross_copy(k)] + list(act_copies(k))
        sends += reduce_copies(k, d_part, d_recv, s_red2, r_red2) + bcast_copies(k, out_all, s_bc2, r_bc2)
        for copy in sends:
            copy.wait_send()
        for copy in out_copies(k):
            copy.wait()


def mlp_call(attn, x_in, gain, w_o, w_gate, w_up, w_down):
    row_total, hid = x_in.shape
    ff = w_gate.shape[1]
    rb = row_total // (4 * CHUNKS)
    bf16 = jnp.bfloat16
    f32 = jnp.float32
    hbm = pl.BlockSpec(memory_space=pltpu.HBM)
    dma = pltpu.SemaphoreType.DMA
    return pl.pallas_call(
        mlp_kernel,
        out_shape=jax.ShapeDtypeStruct((row_total, hid), bf16),
        in_specs=[hbm] * 7,
        out_specs=hbm,
        scratch_shapes=[
            pltpu.VMEM(attn.shape, bf16), pltpu.VMEM((hid // 128, 128), bf16),
            pltpu.VMEM(w_o.shape, bf16), pltpu.VMEM(w_gate.shape, bf16), pltpu.VMEM(w_up.shape, bf16), pltpu.VMEM(w_down.shape, bf16),
            pltpu.VMEM((CHUNKS * rb, hid), bf16),
            pltpu.VMEM((CHUNKS, 4, rb, hid), bf16),
            pltpu.VMEM((CHUNKS, 4, rb, hid), bf16), pltpu.VMEM((CHUNKS, 3, rb, hid), bf16),
            pltpu.VMEM((CHUNKS, 4, rb, hid), bf16),
            pltpu.VMEM((CHUNKS, 8, 128), f32), pltpu.VMEM((CHUNKS, 3, 8, 128), f32),
            pltpu.VMEM((4 * rb, hid), bf16),
            pltpu.VMEM((CHUNKS, 4, rb, 2 * ff), bf16), pltpu.VMEM((CHUNKS, 2, rb, 2 * ff), bf16),
            pltpu.VMEM((CHUNKS, rb, 2 * ff), bf16), pltpu.VMEM((CHUNKS, rb, 2 * ff), bf16),
            pltpu.VMEM((CHUNKS, 4, rb, ff), bf16),
            pltpu.VMEM((4 * rb, hid), f32),
            pltpu.VMEM((CHUNKS, 4, rb, hid), bf16), pltpu.VMEM((CHUNKS, 3, rb, hid), bf16),
            pltpu.VMEM((CHUNKS, 4, rb, hid), bf16),
            dma((7,)),
            dma((CHUNKS, 3)), dma((CHUNKS, 3)), dma((CHUNKS, 3)), dma((CHUNKS, 3)), dma((CHUNKS, 3)), dma((CHUNKS, 3)),
            dma((CHUNKS, 3)), dma((CHUNKS, 3)), dma((CHUNKS, 2)), dma((CHUNKS, 2)),
            dma((CHUNKS,)), dma((CHUNKS,)), dma((CHUNKS, 3)), dma((CHUNKS, 3)),
            dma((CHUNKS, 3)), dma((CHUNKS, 3)), dma((CHUNKS, 3)), dma((CHUNKS, 3)), dma((CHUNKS, 4)),
        ],
        compiler_params=pltpu.CompilerParams(collective_id=1, has_side_effects=True, vmem_limit_bytes=VMEM_BYTES),
        name="attn_out_mlp",
    )(attn, x_in, gain.reshape(-1, 128), w_o, w_gate, w_up, w_down)


def qkv_kernel(x_hbm, seq_hbm, gain_hbm, w_q_hbm, w_k_hbm, w_v_hbm, b_q_hbm, b_k_hbm, b_v_hbm, q_out, k_out, v_out,
               x, seq, gain, w_q, w_k, w_v, b_q, b_k, b_v, load_sem, stat_send, stat_recv, h1, part, pair_recv, cross_send, cross_recv,
               s_stat, r_stat, s_pair, r_pair, s_cross, r_cross):
    mx, sib, across, across_sib = mx_peers()
    rows, hid = x.shape
    block = rows // 4
    q_cols = w_q.shape[1]
    loads = [pltpu.make_async_copy(src, dst, load_sem.at[i]) for i, (src, dst) in enumerate((
        (x_hbm, x), (gain_hbm, gain), (w_q_hbm, w_q), (w_k_hbm, w_k), (w_v_hbm, w_v), (b_q_hbm, b_q), (b_k_hbm, b_k), (b_v_hbm, b_v), (seq_hbm, seq)))]
    for load in loads:
        load.start()
    enter([("mx", sib), ("mx", across), ("mx", across_sib)])
    loads[0].wait()

    def remote(src, dst, send, recv, peer):
        return pltpu.make_async_remote_copy(src_ref=src, dst_ref=dst, send_sem=send, recv_sem=recv, device_id={"mx": peer}, device_id_type=MESH_IDS)

    for j in range(4):
        piece = x[j * block:(j + 1) * block].astype(jnp.float32)
        stat_send[:, j * block:(j + 1) * block] = column_to_lanes(jnp.sum(piece * piece, axis=1, keepdims=True))
    stat_copies = [remote(stat_send, stat_recv.at[d], s_stat.at[d], r_stat.at[d], p) for d, p in enumerate((sib, across, across_sib))]
    for copy in stat_copies:
        copy.start()
    for load in loads[1:]:
        load.wait()
    for copy in stat_copies:
        copy.wait_recv()
    total = stat_send[...] + stat_recv[0] + stat_recv[1] + stat_recv[2]
    stat_recv[0] = lax.rsqrt(total / (4 * hid) + NORM_EPS)
    gain_rows = gain[...].astype(jnp.float32)
    pair_copies = [remote(part.at[across_sib], pair_recv.at[0], s_pair.at[0], r_pair.at[0], sib),
                   remote(part.at[sib], pair_recv.at[1], s_pair.at[1], r_pair.at[1], sib)]
    cross = remote(cross_send, cross_recv, s_cross, r_cross, across)

    def project(j):
        start = pl.multiple_of(j * block, block)
        scale = lanes_to_column(stat_recv[0, :, pl.ds(start, block)])
        for t in range(hid // 128):
            cols = slice(t * 128, (t + 1) * 128)
            h1[:, cols] = (x[pl.ds(start, block), cols].astype(jnp.float32) * scale * gain_rows[t:t + 1]).astype(jnp.bfloat16)
        lhs = h1[...]
        off = 0
        for w in (w_q, w_k, w_v):
            part[j, :, off:off + w.shape[1]] = jnp.dot(lhs, w[...], preferred_element_type=jnp.float32).astype(jnp.bfloat16)
            off += w.shape[1]

    project(across_sib)
    pair_copies[0].start()
    project(across)
    pair_copies[0].wait_recv()
    cross_send[...] = (part[across].astype(jnp.float32) + pair_recv[0].astype(jnp.float32)).astype(jnp.bfloat16)
    cross.start()
    project(sib)
    pair_copies[1].start()
    project(mx)
    lane = lax.broadcasted_iota(jnp.int32, (block, HEAD), 1)
    inv_freq = jnp.exp(lax.rem(lane, HEAD // 2).astype(jnp.float32) * (-2.0 / HEAD * math.log(ROPE_THETA)))
    angles = lanes_to_column(seq[...].astype(jnp.float32)) * inv_freq
    cos_tab = jnp.cos(angles)
    sin_tab = jnp.where(lane < HEAD // 2, -jnp.sin(angles), jnp.sin(angles))
    pair_copies[1].wait_recv()
    cross.wait_recv()

    def total_of(off, bias):
        cols = slice(off, off + HEAD)
        return part[mx, :, cols].astype(jnp.float32) + pair_recv[1, :, cols].astype(jnp.float32) + cross_recv[:, cols].astype(jnp.float32) + bias.astype(jnp.float32)

    def rotated(vals):
        return (vals * cos_tab + pltpu.roll(vals, HEAD // 2, 1) * sin_tab).astype(jnp.bfloat16).astype(jnp.float32)

    heads = q_cols // HEAD
    for h in range(heads):
        q_out[:, h, :] = rotated(total_of(h * HEAD, b_q[h:h + 1]))
    for h in range(heads, q_out.shape[1]):
        q_out[:, h, :] = jnp.zeros((block, HEAD), jnp.float32)
    k_out[...] = rotated(total_of(q_cols, b_k[...]))
    v_out[...] = total_of(q_cols + HEAD, b_v[...]).astype(jnp.bfloat16).astype(jnp.float32)
    for copy in stat_copies + pair_copies + [cross]:
        copy.wait_send()


def qkv_call(x_in, seq_lens, gain, w_q, w_k, w_v, b_q, b_k, b_v):
    rows, hid = x_in.shape
    block = rows // 4
    cols = w_q.shape[1] + w_k.shape[1] + w_v.shape[1]
    heads_pad = -(-w_q.shape[1] // HEAD // 8) * 8
    bf16 = jnp.bfloat16
    f32 = jnp.float32
    vmem = pl.BlockSpec(memory_space=pltpu.VMEM)
    hbm = pl.BlockSpec(memory_space=pltpu.HBM)
    dma = pltpu.SemaphoreType.DMA
    return pl.pallas_call(
        qkv_kernel,
        out_shape=(jax.ShapeDtypeStruct((block, heads_pad, HEAD), f32), jax.ShapeDtypeStruct((block, HEAD), f32), jax.ShapeDtypeStruct((block, HEAD), f32)),
        in_specs=[hbm] * 9,
        out_specs=(vmem, vmem, vmem),
        scratch_shapes=[
            pltpu.VMEM(x_in.shape, bf16), pltpu.VMEM((1, block), jnp.int32), pltpu.VMEM((hid // 128, 128), bf16),
            pltpu.VMEM(w_q.shape, bf16), pltpu.VMEM(w_k.shape, bf16), pltpu.VMEM(w_v.shape, bf16),
            pltpu.VMEM((w_q.shape[1] // HEAD, HEAD), bf16), pltpu.VMEM((1, HEAD), bf16), pltpu.VMEM((1, HEAD), bf16), dma((9,)),
            pltpu.VMEM((8, rows), f32), pltpu.VMEM((3, 8, rows), f32), pltpu.VMEM((block, hid), bf16),
            pltpu.VMEM((4, block, cols), bf16), pltpu.VMEM((2, block, cols), bf16), pltpu.VMEM((block, cols), bf16), pltpu.VMEM((block, cols), bf16),
            dma((3,)), dma((3,)), dma((2,)), dma((2,)), dma, dma,
        ],
        compiler_params=pltpu.CompilerParams(collective_id=0, has_side_effects=True, vmem_limit_bytes=VMEM_BYTES),
        name="norm_qkv",
    )(x_in, seq_lens.reshape(1, block), gain.reshape(-1, 128), w_q, w_k, w_v, b_q.reshape(-1, HEAD), b_k.reshape(1, -1), b_v.reshape(1, -1))


GROUP_ROWS = 4
SLOTS = 8
AHEAD = 4


def attend_kernel(seq_hbm, q_hbm, k_new_hbm, v_new_hbm, k_cache, v_cache, attn_hbm, k_out, v_out, k_buf, v_buf, heads_out, attn, seq, q, k_new, v_new, in_sem, out_sem, misc_sem):
    batch, length, _ = k_cache.shape
    groups = batch // GROUP_ROWS

    def fetch(i):
        slot = lax.rem(i, SLOTS)
        rows = pl.ds(i * GROUP_ROWS, GROUP_ROWS)
        return (pltpu.make_async_copy(k_cache.at[rows], k_buf.at[slot], in_sem.at[0, slot]),
                pltpu.make_async_copy(v_cache.at[rows], v_buf.at[slot], in_sem.at[1, slot]))

    def flush(i):
        slot = lax.rem(i, SLOTS)
        rows = pl.ds(i * GROUP_ROWS, GROUP_ROWS)
        return (pltpu.make_async_copy(k_buf.at[slot], k_out.at[rows], out_sem.at[0, slot]),
                pltpu.make_async_copy(v_buf.at[slot], v_out.at[rows], out_sem.at[1, slot]))

    loads = [pltpu.make_async_copy(src, dst, misc_sem.at[i]) for i, (src, dst) in enumerate(((seq_hbm, seq), (q_hbm, q), (k_new_hbm, k_new), (v_new_hbm, v_new)))]
    for load in loads:
        load.start()
    for i in range(AHEAD):
        for copy in fetch(jnp.int32(i)):
            copy.start()
    for load in loads:
        load.wait()


    def step(i, carry):
        slot = lax.rem(i, SLOTS)
        for copy in fetch(i):
            copy.wait()
        tile_row = lax.broadcasted_iota(jnp.int32, (16, HEAD), 0)
        for r in range(GROUP_ROWS):
            b = i * GROUP_ROWS + r
            pos = seq[b]
            base = pl.multiple_of(pos // 16 * 16, 16)
            hit = tile_row == pos - base
            for buf, new in ((k_buf, k_new), (v_buf, v_new)):
                tile = buf[slot, r, pl.ds(base, 16), :].astype(jnp.float32)
                buf[slot, r, pl.ds(base, 16), :] = jnp.where(hit, new[pl.ds(b, 1), :], tile).astype(jnp.bfloat16)
        scores = []
        for r in range(GROUP_ROWS):
            b = i * GROUP_ROWS + r
            s = lax.dot_general(q[b].astype(jnp.bfloat16), k_buf[slot, r], (((1,), (1,)), ((), ())), preferred_element_type=jnp.float32) * HEAD ** -0.5
            t = lax.broadcasted_iota(jnp.int32, s.shape, 1)
            scores.append(jnp.where(t <= seq[b], s, -jnp.inf))
        for r in range(GROUP_ROWS):
            b = i * GROUP_ROWS + r
            s = scores[r]
            w = jnp.exp(s - jnp.max(s, axis=1, keepdims=True))
            total = jnp.sum(w, axis=1, keepdims=True)
            o = jnp.dot(w.astype(jnp.bfloat16), v_buf[slot, r], preferred_element_type=jnp.float32)
            heads_out[b] = o / total
        for copy in flush(i):
            copy.start()

        @pl.when(i + AHEAD < groups)
        def _():
            @pl.when(i + AHEAD >= SLOTS)
            def _():
                for copy in flush(i + AHEAD - SLOTS):
                    copy.wait()

            for copy in fetch(i + AHEAD):
                copy.start()

        return carry

    lax.fori_loop(0, groups, step, 0)
    for h in range(attn.shape[1] // HEAD):
        attn[:, h * HEAD:(h + 1) * HEAD] = heads_out[:, h, :].astype(jnp.bfloat16)
    attn_store = pltpu.make_async_copy(attn, attn_hbm, misc_sem.at[4])
    attn_store.start()
    for i in range(groups - SLOTS, groups):
        for copy in flush(jnp.int32(i)):
            copy.wait()
    attn_store.wait()


def attend_call(seq_lens, q, k_new, v_new, k_cache, v_cache, q_cols):
    batch, length, _, _ = k_cache.shape
    bf16 = jnp.bfloat16
    f32 = jnp.float32
    hbm = pl.BlockSpec(memory_space=pltpu.HBM)
    dma = pltpu.SemaphoreType.DMA
    flat = (batch, length, HEAD)
    attn, k_out, v_out = pl.pallas_call(
        attend_kernel,
        out_shape=(jax.ShapeDtypeStruct((batch, q_cols), bf16), jax.ShapeDtypeStruct(flat, bf16), jax.ShapeDtypeStruct(flat, bf16)),
        in_specs=[hbm] * 6,
        out_specs=(hbm, hbm, hbm),
        scratch_shapes=[
            pltpu.VMEM((SLOTS, GROUP_ROWS, length, HEAD), bf16), pltpu.VMEM((SLOTS, GROUP_ROWS, length, HEAD), bf16),
            pltpu.VMEM(q.shape, f32), pltpu.VMEM((batch, q_cols), bf16), pltpu.SMEM((batch,), jnp.int32),
            pltpu.VMEM(q.shape, f32), pltpu.VMEM(k_new.shape, f32), pltpu.VMEM(v_new.shape, f32),
            dma((2, SLOTS)), dma((2, SLOTS)), dma((5,)),
        ],
        compiler_params=pltpu.CompilerParams(vmem_limit_bytes=VMEM_BYTES),
        name="attend_and_update",
    )(seq_lens, q, k_new, v_new, k_cache.reshape(flat), v_cache.reshape(flat))
    return attn, k_out.reshape(k_cache.shape), v_out.reshape(v_cache.shape)


def solution(mesh):
    act_spec = P(None, "mx")
    cache_spec = P("mx", None, "my", None)
    in_specs = (act_spec, P("mx"), P("mx"), P("mx"), P("mx", "my"), P("my"), P("mx", "my"), P("my"), P("mx", "my"), P("my"), P("my", "mx"), P("mx", "my"), P("mx", "my"), P("my", "mx"), cache_spec, cache_spec)
    out_specs = (act_spec, cache_spec, cache_spec)

    def local_layer(x_in, seq_lens, gain_attn, gain_mlp, w_q, b_q, w_k, b_k, w_v, b_v, w_o, w_gate, w_up, w_down, k_cache, v_cache):
        q, k_new, v_new = qkv_call(x_in, seq_lens, gain_attn, w_q, w_k, w_v, b_q, b_k, b_v)
        attn, k_cache_out, v_cache_out = attend_call(seq_lens, q, k_new, v_new, k_cache, v_cache, w_q.shape[1])
        x_out = mlp_call(attn, x_in, gain_mlp, w_o, w_gate, w_up, w_down)
        return x_out, k_cache_out, v_cache_out

    return jax.shard_map(local_layer, mesh=mesh, in_specs=in_specs, out_specs=out_specs, check_vma=False)
```

```python
import math

import jax
import jax.numpy as jnp
from jax import lax
from jax.experimental import pallas as pl
from jax.experimental.pallas import tpu as pltpu
from jax.sharding import PartitionSpec as P

HEAD = 128
NORM_EPS = 1e-6
ROPE_THETA = 1000000.0
VMEM_BYTES = 67043328
MLP_VMEM_BYTES = 65900000
CHUNK_ROWS = (16, 32, 32, 32, 16)
CHUNK_STARTS = (0, 16, 48, 80, 112)
SPAN_TILES = (12, 12, 13)
PLAN = ((0, 0, 0), (1, 0, 0), (0, 1, 0), (0, 2, 0), (1, 1, 0), (0, 3, 0), (0, 4, 0), (2, 0, 0), (1, 2, 0), (1, 3, 0), (1, 4, 0), (2, 1, 0), (3, 0, 0), (2, 2, 0), (4, 0, 0), (4, 0, 1), (5, 0, 0), (4, 0, 2), (5, 0, 1), (3, 1, 0), (5, 0, 2), (2, 3, 0), (6, 0, 0), (4, 1, 0), (6, 0, 1), (4, 1, 1), (5, 1, 0), (7, 0, 0), (7, 0, 1), (5, 1, 1), (6, 0, 2), (8, 0, 0), (8, 0, 1), (4, 1, 2), (6, 1, 0), (3, 2, 0), (5, 1, 2), (3, 3, 0), (4, 2, 0), (7, 0, 2), (5, 2, 0), (8, 0, 2), (7, 1, 0), (6, 1, 1), (8, 1, 0), (4, 2, 1), (6, 1, 2), (5, 2, 1), (4, 2, 2), (6, 2, 0), (5, 2, 2), (9, 0, 0), (4, 3, 0), (7, 1, 1), (4, 3, 1), (7, 1, 2), (8, 1, 1), (5, 3, 0), (8, 1, 2), (5, 3, 1), (4, 3, 2), (6, 2, 1), (2, 4, 0), (5, 3, 2), (7, 2, 0), (10, 0, 0), (8, 2, 0), (3, 4, 0), (9, 1, 0), (6, 2, 2), (4, 4, 0), (4, 4, 1), (5, 4, 0), (6, 3, 0), (5, 4, 1), (4, 4, 2), (10, 1, 0), (5, 4, 2), (6, 3, 1), (7, 2, 1), (8, 2, 1), (6, 3, 2), (7, 2, 2), (8, 2, 2), (6, 4, 0), (7, 3, 0), (8, 3, 0), (6, 4, 1), (9, 2, 0), (6, 4, 2), (7, 3, 1), (8, 3, 1), (7, 3, 2), (7, 4, 0), (7, 4, 1), (8, 3, 2), (7, 4, 2), (8, 4, 0), (8, 4, 1), (8, 4, 2), (10, 2, 0), (9, 3, 0), (9, 4, 0), (10, 3, 0), (10, 4, 0))
MESH_IDS = pl.DeviceIdType.MESH


def in_hbm(array):
    return pltpu.with_memory_space_constraint(array, pltpu.HBM)


def in_vmem(array):
    return pltpu.with_memory_space_constraint(array, pltpu.VMEM)


def over_tiles(total, tile, body):
    count = total // tile

    def step(i, carry):
        body(pl.multiple_of(i * tile, tile), tile)
        return carry

    lax.fori_loop(0, count, step, 0)
    if total % tile:
        body(count * tile, total % tile)


def mx_peers():
    me = lax.axis_index("mx")
    core = lax.rem(me, 2)
    sib = me + 1 - 2 * core
    return me, sib, lax.rem(me + 2, 4), lax.rem(sib + 2, 4)


def my_peers():
    me = lax.axis_index("my")
    flip = me + 1 - 2 * lax.rem(me, 2)
    return me, (flip, lax.rem(me + 2, 4), lax.rem(flip + 2, 4))


def column_to_lanes(col):
    wide = jnp.broadcast_to(col, (col.shape[0], 128))
    if col.shape[0] < 128:
        wide = jnp.concatenate([wide] * (128 // col.shape[0]), axis=0)
    return jnp.transpose(wide)[:8]


def lanes_to_column(lanes):
    return jnp.transpose(jnp.broadcast_to(lanes[:1], (128, 128)))


def enter(axis_peers):
    barrier = pltpu.get_barrier_semaphore()
    for axis, peer in axis_peers:
        pl.semaphore_signal(barrier, inc=1, device_id={axis: peer}, device_id_type=MESH_IDS)
    pl.semaphore_wait(barrier, len(axis_peers))


def mlp_kernel(attn_hbm, x_in, gain_hbm, w_o, w_gate, w_up, w_down, out,
               attn, gain, wo_v, wg_v, wu_v, wd_v, x_v, attn_all, o_part, o_recv, mid, stat_send, stat_recv, h2,
               part, pair_recv, cross_send, cross_recv, act, acc, d_part, d_recv,
               w_sem, s_gather, r_gather, s_red, r_red, s_bc, r_bc, s_stat, r_stat, s_pair, r_pair,
               s_cross, r_cross, s_act, r_act, s_red2, r_red2, s_bc2, r_bc2):
    mx, sib, across, across_sib = mx_peers()
    my, my_list = my_peers()
    block = attn.shape[0]
    hid = mid.shape[2]
    ff = wg_v.shape[1]
    chunks = len(CHUNK_ROWS)
    spans = []
    for tiles in SPAN_TILES:
        start = spans[-1][1] if spans else 0
        spans.append((start, start + tiles * (ff // sum(SPAN_TILES))))

    def rows_of(k):
        return pl.ds(CHUNK_STARTS[k], CHUNK_ROWS[k])

    def pair_cols(h):
        return pl.ds(2 * spans[h][0], 2 * (spans[h][1] - spans[h][0]))

    def span_cols(h):
        return pl.ds(spans[h][0], spans[h][1] - spans[h][0])

    def remote(src, dst, send, recv, axis, peer):
        return pltpu.make_async_remote_copy(src_ref=src, dst_ref=dst, send_sem=send, recv_sem=recv, device_id={axis: peer}, device_id_type=MESH_IDS)

    first_loads = [pltpu.make_async_copy(attn_hbm, attn, w_sem.at[5]), pltpu.make_async_copy(gain_hbm, gain, w_sem.at[6])]
    loads = [
        pltpu.make_async_copy(w_o, wo_v, w_sem.at[0]),
        pltpu.make_async_copy(x_in.at[pl.ds(pl.multiple_of(my * block, block), block)], x_v, w_sem.at[1]),
        pltpu.make_async_copy(w_gate, wg_v, w_sem.at[2]),
        pltpu.make_async_copy(w_up, wu_v, w_sem.at[3]),
        pltpu.make_async_copy(w_down, wd_v, w_sem.at[4]),
    ]
    for load in first_loads + loads:
        load.start()
    enter([("mx", sib), ("mx", across), ("mx", across_sib)] + [("my", p) for p in my_list])

    def gather_to_across(k):
        return remote(attn.at[rows_of(k)], attn_all.at[mx, rows_of(k)], s_gather.at[k, 0], r_gather.at[k, 0], "mx", across)

    def gather_to_sib(k):
        return remote(attn.at[rows_of(k)], attn_all.at[mx, rows_of(k)], s_gather.at[k, 1], r_gather.at[k, 1], "mx", sib)

    def gather_forward(k):
        return remote(attn_all.at[across, rows_of(k)], attn_all.at[across, rows_of(k)], s_gather.at[k, 2], r_gather.at[k, 2], "mx", sib)

    def reduce_copies(k, src, dst, send, recv):
        return [remote(src.at[p, rows_of(k)], dst.at[d, rows_of(k)], send.at[k, d], recv.at[k, d], "my", p) for d, p in enumerate(my_list)]

    def bcast_copies(k, buf, send, recv):
        return [remote(buf.at[my, rows_of(k)], buf.at[my, rows_of(k)], send.at[k, d], recv.at[k, d], "my", p) for d, p in enumerate(my_list)]

    def out_bcast(k):
        rows = pl.ds(pl.multiple_of(my * block + CHUNK_STARTS[k], 16), CHUNK_ROWS[k])
        return [remote(out.at[rows], out.at[rows], s_bc2.at[k, d], r_bc2.at[k, d], "my", p) for d, p in enumerate(my_list)]

    def stat_copies(k):
        return [remote(stat_send.at[k], stat_recv.at[k, d], s_stat.at[k, d], r_stat.at[k, d], "mx", p) for d, p in enumerate((sib, across, across_sib))]

    def pair_first(k, h):
        return remote(part.at[across_sib, rows_of(k), pair_cols(h)], pair_recv.at[0, rows_of(k), pair_cols(h)], s_pair.at[k, 2 * h], r_pair.at[k, 2 * h], "mx", sib)

    def pair_second(k, h):
        return remote(part.at[sib, rows_of(k), pair_cols(h)], pair_recv.at[1, rows_of(k), pair_cols(h)], s_pair.at[k, 2 * h + 1], r_pair.at[k, 2 * h + 1], "mx", sib)

    def cross_copy(k, h):
        return remote(cross_send.at[rows_of(k), pair_cols(h)], cross_recv.at[rows_of(k), pair_cols(h)], s_cross.at[k, h], r_cross.at[k, h], "mx", across)

    def act_copy(k, h, which):
        owner, peer = ((mx, across), (mx, sib), (across, sib))[which]
        ref = act.at[owner, rows_of(k), span_cols(h)]
        return remote(ref, ref, s_act.at[k, 3 * h + which], r_act.at[k, 3 * h + which], "mx", peer)

    def forward_gather(k, h):
        gather_to_across(k).wait_recv()
        gather_forward(k).start()

    def out_proj(k, h):
        rb = CHUNK_ROWS[k]
        gather_to_sib(k).wait_recv()
        gather_forward(k).wait_recv()
        if k == 0:
            loads[0].wait()
        rows_in = attn_all[:, rows_of(k), :].reshape(4 * rb, hid)
        o_part[:, rows_of(k), :] = jnp.dot(rows_in, wo_v[...], preferred_element_type=jnp.float32).astype(jnp.bfloat16).reshape(4, rb, hid)
        for copy in reduce_copies(k, o_part, o_recv, s_red, r_red):
            copy.start()

    def own_block(k, h):
        for copy in reduce_copies(k, o_part, o_recv, s_red, r_red):
            copy.wait_recv()
        if k == 0:
            loads[1].wait()
        total = o_part[my, rows_of(k), :].astype(jnp.float32)
        for d in range(3):
            total += o_recv[d, rows_of(k), :].astype(jnp.float32)
        mid[my, rows_of(k), :] = (x_v[rows_of(k), :].astype(jnp.float32) + total).astype(jnp.bfloat16)
        for copy in bcast_copies(k, mid, s_bc, r_bc):
            copy.start()

    def stats(k, h):
        for copy in bcast_copies(k, mid, s_bc, r_bc):
            copy.wait_recv()
        rows_f32 = mid[:, rows_of(k), :].reshape(4 * CHUNK_ROWS[k], hid).astype(jnp.float32)
        stat_send[k] = column_to_lanes(jnp.sum(rows_f32 * rows_f32, axis=1, keepdims=True))
        for copy in stat_copies(k):
            copy.start()

    def gate_up(k, h):
        rb = CHUNK_ROWS[k]
        rows = 4 * rb
        if h == 0:
            for copy in stat_copies(k):
                copy.wait_recv()
            total = stat_send[k] + stat_recv[k, 0] + stat_recv[k, 1] + stat_recv[k, 2]
            scale = lanes_to_column(lax.rsqrt(total / (4 * hid) + NORM_EPS))[:rows]
            gain_rows = gain[...].astype(jnp.float32)
            for t in range(hid // 128):
                cols = slice(t * 128, (t + 1) * 128)
                piece = mid[:, rows_of(k), cols].reshape(rows, 128).astype(jnp.float32)
                h2[k % 2, :rows, cols] = (piece * scale * gain_rows[t:t + 1]).astype(jnp.bfloat16)
            if k == 0:
                loads[2].wait()
                loads[3].wait()
        start, stop = spans[h]

        def body(off, tile):
            lhs = h2[k % 2, :rows, :]
            for w, base in ((wg_v, 2 * start), (wu_v, start + stop)):
                weights = w[:, pl.ds(pl.multiple_of(start + off, 128), tile)]
                part[:, rows_of(k), pl.ds(pl.multiple_of(base + off, 128), tile)] = jnp.dot(lhs, weights, preferred_element_type=jnp.float32).astype(jnp.bfloat16).reshape(4, rb, tile)

        over_tiles(stop - start, 512, body)
        pair_first(k, h).start()
        pair_second(k, h).start()

    def pair_sum(k, h):
        pair_first(k, h).wait_recv()

        def body(off, tile):
            cols = pl.ds(pl.multiple_of(2 * spans[h][0] + off, 128), tile)
            cross_send[rows_of(k), cols] = (part[across, rows_of(k), cols].astype(jnp.float32) + pair_recv[0, rows_of(k), cols].astype(jnp.float32)).astype(jnp.bfloat16)

        over_tiles(2 * (spans[h][1] - spans[h][0]), 512, body)
        cross_copy(k, h).start()

    def activate(k, h):
        pair_second(k, h).wait_recv()
        cross_copy(k, h).wait_recv()
        start, stop = spans[h]

        def total(base, tile):
            cols = pl.ds(pl.multiple_of(base, 128), tile)
            return part[mx, rows_of(k), cols].astype(jnp.float32) + pair_recv[1, rows_of(k), cols].astype(jnp.float32) + cross_recv[rows_of(k), cols].astype(jnp.float32)

        def body(off, tile):
            gate = total(2 * start + off, tile)
            up = total(start + stop + off, tile)
            act[mx, rows_of(k), pl.ds(pl.multiple_of(start + off, 128), tile)] = (jax.nn.silu(gate) * up).astype(jnp.bfloat16)

        over_tiles(stop - start, 512, body)
        act_copy(k, h, 0).start()
        act_copy(k, h, 1).start()

    def forward_act(k, h):
        act_copy(k, h, 0).wait_recv()
        act_copy(k, h, 2).start()

    def down(k, h):
        rb = CHUNK_ROWS[k]
        rows = pl.ds(4 * CHUNK_STARTS[k], 4 * rb)
        act_copy(k, h, 1).wait_recv()
        act_copy(k, h, 2).wait_recv()
        if h == 0:
            if k == 0:
                loads[4].wait()
            acc[rows, :] = jnp.zeros((4 * rb, hid), jnp.float32)
        start, stop = spans[h]

        def body(off, tile):
            cols = pl.ds(pl.multiple_of(start + off, 128), tile)
            lhs = act[:, rows_of(k), cols].reshape(4 * rb, tile)
            acc[rows, :] += jnp.dot(lhs, wd_v[cols, :], preferred_element_type=jnp.float32)

        over_tiles(stop - start, 512, body)
        if h == len(spans) - 1:
            d_part[:, rows_of(k), :] = acc[rows, :].astype(jnp.bfloat16).reshape(4, rb, hid)
            for copy in reduce_copies(k, d_part, d_recv, s_red2, r_red2):
                copy.start()

    def out_block(k, h):
        for copy in reduce_copies(k, d_part, d_recv, s_red2, r_red2):
            copy.wait_recv()
        total = d_part[my, rows_of(k), :].astype(jnp.float32)
        for d in range(3):
            total += d_recv[d, rows_of(k), :].astype(jnp.float32)
        rows = pl.ds(pl.multiple_of(my * block + CHUNK_STARTS[k], 16), CHUNK_ROWS[k])
        out[rows, :] = (mid[my, rows_of(k), :].astype(jnp.float32) + total).astype(jnp.bfloat16)
        for copy in out_bcast(k):
            copy.start()

    def finish(k, h):
        for copy in out_bcast(k):
            copy.wait_recv()

    for load in first_loads:
        load.wait()
    for k in range(chunks):
        gather_to_across(k).start()
        gather_to_sib(k).start()
        attn_all[mx, rows_of(k), :] = attn[rows_of(k), :]
    stages = (forward_gather, out_proj, own_block, stats, gate_up, pair_sum, activate, forward_act, down, out_block, finish)
    for stage, k, h in PLAN:
        stages[stage](k, h)

    for k in range(chunks):
        sends = [gather_to_across(k), gather_to_sib(k), gather_forward(k)] + reduce_copies(k, o_part, o_recv, s_red, r_red) + bcast_copies(k, mid, s_bc, r_bc)
        sends += stat_copies(k) + reduce_copies(k, d_part, d_recv, s_red2, r_red2) + out_bcast(k)
        for h in range(len(spans)):
            sends += [pair_first(k, h), pair_second(k, h), cross_copy(k, h)] + [act_copy(k, h, which) for which in range(3)]
        for copy in sends:
            copy.wait_send()


def mlp_call(attn, x_in, gain, w_o, w_gate, w_up, w_down):
    row_total, hid = x_in.shape
    ff = w_gate.shape[1]
    block = row_total // 4
    chunks = len(CHUNK_ROWS)
    spans = len(SPAN_TILES)
    bf16 = jnp.bfloat16
    f32 = jnp.float32
    hbm = pl.BlockSpec(memory_space=pltpu.HBM)
    dma = pltpu.SemaphoreType.DMA
    four = pltpu.VMEM((4, block, hid), bf16)
    three = pltpu.VMEM((3, block, hid), bf16)
    return pl.pallas_call(
        mlp_kernel,
        out_shape=pltpu.VMEM((row_total, hid), bf16),
        in_specs=[hbm] * 7,
        out_specs=pl.BlockSpec(memory_space=pltpu.VMEM),
        scratch_shapes=[
            pltpu.VMEM(attn.shape, bf16), pltpu.VMEM((hid // 128, 128), bf16),
            pltpu.VMEM(w_o.shape, bf16), pltpu.VMEM(w_gate.shape, bf16), pltpu.VMEM(w_up.shape, bf16), pltpu.VMEM(w_down.shape, bf16),
            pltpu.VMEM((block, hid), bf16),
            four, four, three, four,
            pltpu.VMEM((chunks, 8, 128), f32), pltpu.VMEM((chunks, 3, 8, 128), f32),
            pltpu.VMEM((2, 4 * max(CHUNK_ROWS), hid), bf16),
            pltpu.VMEM((4, block, 2 * ff), bf16), pltpu.VMEM((2, block, 2 * ff), bf16),
            pltpu.VMEM((block, 2 * ff), bf16), pltpu.VMEM((block, 2 * ff), bf16),
            pltpu.VMEM((4, block, ff), bf16),
            pltpu.VMEM((4 * block, hid), f32),
            four, three,
            dma((7,)),
            dma((chunks, 3)), dma((chunks, 3)), dma((chunks, 3)), dma((chunks, 3)), dma((chunks, 3)), dma((chunks, 3)),
            dma((chunks, 3)), dma((chunks, 3)), dma((chunks, 2 * spans)), dma((chunks, 2 * spans)),
            dma((chunks, spans)), dma((chunks, spans)), dma((chunks, 3 * spans)), dma((chunks, 3 * spans)),
            dma((chunks, 3)), dma((chunks, 3)), dma((chunks, 3)), dma((chunks, 3)),
        ],
        compiler_params=pltpu.CompilerParams(collective_id=1, has_side_effects=True, vmem_limit_bytes=MLP_VMEM_BYTES),
        name="attn_out_mlp",
    )(*[in_hbm(a) for a in (attn, x_in, gain.reshape(-1, 128), w_o, w_gate, w_up, w_down)])


QKV_VMEM_BYTES = 9 * 1024 * 1024
ATTEND_VMEM_BYTES = 11 * 1024 * 1024


def qkv_kernel(x_hbm, seq_hbm, gain_hbm, w_q_hbm, w_k_hbm, w_v_hbm, b_q_hbm, b_k_hbm, b_v_hbm, k_cache, v_cache, q_out, k_out, v_out, k_held, v_held,
               x, seq, gain, w_q, w_k, w_v, b_q, b_k, b_v, load_sem, stat_send, stat_recv, h1, part, pair_recv, cross_send, cross_recv,
               s_stat, r_stat, s_pair, r_pair, s_cross, r_cross):
    mx, sib, across, across_sib = mx_peers()
    rows, hid = x.shape
    block = rows // 4
    q_cols = w_q.shape[1]
    loads = [pltpu.make_async_copy(src, dst, load_sem.at[i]) for i, (src, dst) in enumerate((
        (x_hbm, x), (gain_hbm, gain), (w_q_hbm, w_q), (w_k_hbm, w_k), (w_v_hbm, w_v), (b_q_hbm, b_q), (b_k_hbm, b_k), (b_v_hbm, b_v), (seq_hbm, seq)))]
    for load in loads:
        load.start()
    held = [pltpu.make_async_copy(src.at[pl.ds(0, dst.shape[0])], dst, load_sem.at[9 + i]) for i, (src, dst) in enumerate(((k_cache, k_held), (v_cache, v_held)))]
    for load in held:
        load.start()
    enter([("mx", sib), ("mx", across), ("mx", across_sib)])
    loads[0].wait()

    def remote(src, dst, send, recv, peer):
        return pltpu.make_async_remote_copy(src_ref=src, dst_ref=dst, send_sem=send, recv_sem=recv, device_id={"mx": peer}, device_id_type=MESH_IDS)

    for j in range(4):
        piece = x[j * block:(j + 1) * block].astype(jnp.float32)
        stat_send[:, j * block:(j + 1) * block] = column_to_lanes(jnp.sum(piece * piece, axis=1, keepdims=True))
    stat_copies = [remote(stat_send, stat_recv.at[d], s_stat.at[d], r_stat.at[d], p) for d, p in enumerate((sib, across, across_sib))]
    for copy in stat_copies:
        copy.start()
    for load in loads[1:]:
        load.wait()
    for copy in stat_copies:
        copy.wait_recv()
    total = stat_send[...] + stat_recv[0] + stat_recv[1] + stat_recv[2]
    stat_recv[0] = lax.rsqrt(total / (4 * hid) + NORM_EPS)
    gain_rows = gain[...].astype(jnp.float32)
    pair_copies = [remote(part.at[across_sib], pair_recv.at[0], s_pair.at[0], r_pair.at[0], sib),
                   remote(part.at[sib], pair_recv.at[1], s_pair.at[1], r_pair.at[1], sib)]
    cross = remote(cross_send, cross_recv, s_cross, r_cross, across)

    def project(j):
        start = pl.multiple_of(j * block, block)
        scale = lanes_to_column(stat_recv[0, :, pl.ds(start, block)])
        for t in range(hid // 128):
            cols = slice(t * 128, (t + 1) * 128)
            h1[:, cols] = (x[pl.ds(start, block), cols].astype(jnp.float32) * scale * gain_rows[t:t + 1]).astype(jnp.bfloat16)
        lhs = h1[...]
        off = 0
        for w in (w_q, w_k, w_v):
            part[j, :, off:off + w.shape[1]] = jnp.dot(lhs, w[...], preferred_element_type=jnp.float32).astype(jnp.bfloat16)
            off += w.shape[1]

    project(across_sib)
    pair_copies[0].start()
    project(across)
    pair_copies[0].wait_recv()
    cross_send[...] = (part[across].astype(jnp.float32) + pair_recv[0].astype(jnp.float32)).astype(jnp.bfloat16)
    cross.start()
    project(sib)
    pair_copies[1].start()
    project(mx)
    lane = lax.broadcasted_iota(jnp.int32, (block, HEAD), 1)
    inv_freq = jnp.exp(lax.rem(lane, HEAD // 2).astype(jnp.float32) * (-2.0 / HEAD * math.log(ROPE_THETA)))
    angles = lanes_to_column(seq[...].astype(jnp.float32)) * inv_freq
    cos_tab = jnp.cos(angles)
    sin_tab = jnp.where(lane < HEAD // 2, -jnp.sin(angles), jnp.sin(angles))
    pair_copies[1].wait_recv()
    cross.wait_recv()

    def total_of(off, bias):
        cols = slice(off, off + HEAD)
        return part[mx, :, cols].astype(jnp.float32) + pair_recv[1, :, cols].astype(jnp.float32) + cross_recv[:, cols].astype(jnp.float32) + bias.astype(jnp.float32)

    def rotated(vals):
        return (vals * cos_tab + pltpu.roll(vals, HEAD // 2, 1) * sin_tab).astype(jnp.bfloat16).astype(jnp.float32)

    heads = q_cols // HEAD
    for h in range(heads):
        q_out[:, h, :] = rotated(total_of(h * HEAD, b_q[h:h + 1]))
    for h in range(heads, q_out.shape[1]):
        q_out[:, h, :] = jnp.zeros((block, HEAD), jnp.float32)
    k_out[...] = rotated(total_of(q_cols, b_k[...]))
    v_out[...] = total_of(q_cols + HEAD, b_v[...]).astype(jnp.bfloat16).astype(jnp.float32)
    for copy in stat_copies + pair_copies + [cross]:
        copy.wait_send()
    for load in held:
        load.wait()


def qkv_call(x_in, seq_lens, gain, w_q, w_k, w_v, b_q, b_k, b_v, k_cache, v_cache):
    rows, hid = x_in.shape
    block = rows // 4
    cols = w_q.shape[1] + w_k.shape[1] + w_v.shape[1]
    held = pltpu.VMEM((HELD_ROWS,) + k_cache.shape[1:], jnp.bfloat16)
    heads_pad = -(-w_q.shape[1] // HEAD // 8) * 8
    bf16 = jnp.bfloat16
    f32 = jnp.float32
    vmem = pl.BlockSpec(memory_space=pltpu.VMEM)
    hbm = pl.BlockSpec(memory_space=pltpu.HBM)
    dma = pltpu.SemaphoreType.DMA
    return pl.pallas_call(
        qkv_kernel,
        out_shape=(pltpu.VMEM((block, heads_pad, HEAD), f32), pltpu.VMEM((block, HEAD), f32), pltpu.VMEM((block, HEAD), f32), held, held),
        in_specs=[hbm] * 11,
        out_specs=(vmem,) * 5,
        scratch_shapes=[
            pltpu.VMEM(x_in.shape, bf16), pltpu.VMEM((1, block), jnp.int32), pltpu.VMEM((hid // 128, 128), bf16),
            pltpu.VMEM(w_q.shape, bf16), pltpu.VMEM(w_k.shape, bf16), pltpu.VMEM(w_v.shape, bf16),
            pltpu.VMEM((w_q.shape[1] // HEAD, HEAD), bf16), pltpu.VMEM((1, HEAD), bf16), pltpu.VMEM((1, HEAD), bf16), dma((11,)),
            pltpu.VMEM((8, rows), f32), pltpu.VMEM((3, 8, rows), f32), pltpu.VMEM((block, hid), bf16),
            pltpu.VMEM((4, block, cols), bf16), pltpu.VMEM((2, block, cols), bf16), pltpu.VMEM((block, cols), bf16), pltpu.VMEM((block, cols), bf16),
            dma((3,)), dma((3,)), dma((2,)), dma((2,)), dma, dma,
        ],
        compiler_params=pltpu.CompilerParams(collective_id=0, has_side_effects=True, vmem_limit_bytes=QKV_VMEM_BYTES),
        name="norm_qkv",
    )(*[in_hbm(a) for a in (x_in, seq_lens.reshape(1, block), gain.reshape(-1, 128), w_q, w_k, w_v, b_q.reshape(-1, HEAD), b_k.reshape(1, -1), b_v.reshape(1, -1), k_cache, v_cache)])


HELD_ROWS = 96
GROUP_ROWS = 4
SLOTS = 8


def attend_kernel(seq_hbm, q, k_new, v_new, k_held, v_held, k_cache, v_cache, attn_hbm, k_out, v_out, k_buf, v_buf, heads_out, attn, seq, in_sem, out_sem, held_sem, misc_sem):
    batch, length, _ = k_cache.shape
    held_groups = HELD_ROWS // GROUP_ROWS
    fetched = (batch - HELD_ROWS) // GROUP_ROWS
    seq_load = pltpu.make_async_copy(seq_hbm, seq, misc_sem.at[0])
    seq_load.start()

    def rows_of(i):
        return pl.ds(i * GROUP_ROWS, GROUP_ROWS)

    def fetch(i):
        slot = lax.rem(i, SLOTS)
        return (pltpu.make_async_copy(k_cache.at[rows_of(i + held_groups)], k_buf.at[slot], in_sem.at[0, slot]),
                pltpu.make_async_copy(v_cache.at[rows_of(i + held_groups)], v_buf.at[slot], in_sem.at[1, slot]))

    def flush(i):
        slot = lax.rem(i, SLOTS)
        return (pltpu.make_async_copy(k_buf.at[slot], k_out.at[rows_of(i + held_groups)], out_sem.at[0, slot]),
                pltpu.make_async_copy(v_buf.at[slot], v_out.at[rows_of(i + held_groups)], out_sem.at[1, slot]))

    def flush_held(i):
        return (pltpu.make_async_copy(k_held.at[rows_of(i)], k_out.at[rows_of(i)], held_sem.at[0]),
                pltpu.make_async_copy(v_held.at[rows_of(i)], v_out.at[rows_of(i)], held_sem.at[1]))

    def attend(first, k_group, v_group):
        tile_row = lax.broadcasted_iota(jnp.int32, (16, HEAD), 0)
        for r in range(GROUP_ROWS):
            b = first + r
            pos = seq[b]
            base = pl.multiple_of(pos // 16 * 16, 16)
            hit = tile_row == pos - base
            for group, new in ((k_group, k_new), (v_group, v_new)):
                tile = group[r, pl.ds(base, 16), :].astype(jnp.float32)
                group[r, pl.ds(base, 16), :] = jnp.where(hit, new[pl.ds(b, 1), :], tile).astype(jnp.bfloat16)
        scores = []
        for r in range(GROUP_ROWS):
            b = first + r
            s = lax.dot_general(q[b].astype(jnp.bfloat16), k_group[r], (((1,), (1,)), ((), ())), preferred_element_type=jnp.float32) * HEAD ** -0.5
            t = lax.broadcasted_iota(jnp.int32, s.shape, 1)
            scores.append(jnp.where(t <= seq[b], s, -jnp.inf))
        for r in range(GROUP_ROWS):
            s = scores[r]
            w = jnp.exp(s - jnp.max(s, axis=1, keepdims=True))
            total = jnp.sum(w, axis=1, keepdims=True)
            o = jnp.dot(w.astype(jnp.bfloat16), v_group[r], preferred_element_type=jnp.float32)
            heads_out[first + r] = o / total

    for i in range(SLOTS):
        for copy in fetch(jnp.int32(i)):
            copy.start()
    seq_load.wait()

    def held_step(i, carry):
        attend(i * GROUP_ROWS, k_held.at[rows_of(i)], v_held.at[rows_of(i)])
        for copy in flush_held(i):
            copy.start()
        return carry

    def fetched_step(i, carry):
        slot = lax.rem(i, SLOTS)
        for copy in fetch(i):
            copy.wait()
        attend((i + held_groups) * GROUP_ROWS, k_buf.at[slot], v_buf.at[slot])
        for copy in flush(i):
            copy.start()
        return carry

    lax.fori_loop(0, held_groups, held_step, 0)
    lax.fori_loop(0, fetched, fetched_step, 0)
    for h in range(attn.shape[1] // HEAD):
        attn[:, h * HEAD:(h + 1) * HEAD] = heads_out[:, h, :].astype(jnp.bfloat16)
    attn_store = pltpu.make_async_copy(attn, attn_hbm, misc_sem.at[1])
    attn_store.start()
    for src, dst, sem in ((k_held, k_out, held_sem.at[0]), (v_held, v_out, held_sem.at[1])):
        pltpu.make_async_copy(src, dst.at[pl.ds(0, HELD_ROWS)], sem).wait()
    for i in range(fetched):
        for copy in flush(jnp.int32(i)):
            copy.wait()
    attn_store.wait()


def attend_call(seq_lens, q, k_new, v_new, k_held, v_held, k_cache, v_cache, q_cols):
    batch, length, _ = k_cache.shape
    bf16 = jnp.bfloat16
    f32 = jnp.float32
    vmem = pl.BlockSpec(memory_space=pltpu.VMEM)
    hbm = pl.BlockSpec(memory_space=pltpu.HBM)
    dma = pltpu.SemaphoreType.DMA
    return pl.pallas_call(
        attend_kernel,
        out_shape=(pltpu.HBM((batch, q_cols), bf16), jax.ShapeDtypeStruct(k_cache.shape, bf16), jax.ShapeDtypeStruct(k_cache.shape, bf16)),
        in_specs=[hbm] + [vmem] * 5 + [hbm] * 2,
        out_specs=(hbm, hbm, hbm),
        scratch_shapes=[
            pltpu.VMEM((SLOTS, GROUP_ROWS, length, HEAD), bf16), pltpu.VMEM((SLOTS, GROUP_ROWS, length, HEAD), bf16),
            pltpu.VMEM(q.shape, f32), pltpu.VMEM((batch, q_cols), bf16), pltpu.SMEM((batch,), jnp.int32),
            dma((2, SLOTS)), dma((2, SLOTS)), dma((2,)), dma((2,)),
        ],
        compiler_params=pltpu.CompilerParams(vmem_limit_bytes=ATTEND_VMEM_BYTES),
        name="attend_and_update",
    )(in_hbm(seq_lens), *[in_vmem(a) for a in (q, k_new, v_new, k_held, v_held)], in_hbm(k_cache), in_hbm(v_cache))


def solution(mesh):
    act_spec = P(None, "mx")
    cache_spec = P("mx", None, "my", None)
    in_specs = (act_spec, P("mx"), P("mx"), P("mx"), P("mx", "my"), P("my"), P("mx", "my"), P("my"), P("mx", "my"), P("my"), P("my", "mx"), P("mx", "my"), P("mx", "my"), P("my", "mx"), cache_spec, cache_spec)
    out_specs = (act_spec, cache_spec, cache_spec)

    def local_layer(x_in, seq_lens, gain_attn, gain_mlp, w_q, b_q, w_k, b_k, w_v, b_v, w_o, w_gate, w_up, w_down, k_cache, v_cache):
        k_flat = k_cache.reshape(k_cache.shape[:2] + (HEAD,))
        v_flat = v_cache.reshape(k_flat.shape)
        q, k_new, v_new, k_held, v_held = qkv_call(x_in, seq_lens, gain_attn, w_q, w_k, w_v, b_q, b_k, b_v, k_flat, v_flat)
        attn, k_out, v_out = attend_call(seq_lens, q, k_new, v_new, k_held, v_held, k_flat, v_flat, w_q.shape[1])
        x_out = mlp_call(attn, x_in, gain_mlp, w_o, w_gate, w_up, w_down)
        return x_out, k_out.reshape(k_cache.shape), v_out.reshape(v_cache.shape)

    return jax.shard_map(local_layer, mesh=mesh, in_specs=in_specs, out_specs=out_specs, check_vma=False)
```
